32 devices in a mesh: dp: 8 (over y, x, core), expert: 4 (over z).
Axes of the slice: x: 2, y: 2, z: 4, core: 2. Of those that a mesh axis runs over, the one named last changes fastest.
Arguments:
- hidden_states: bfloat16 [4, 8192, 4096], P(None, ('dp', 'expert')), may hold values from -8 to 8
- router_weight: bfloat16 [4, 8, 4096], replicated, may hold values from -0.125 to 0.125
- expert_ids: int32 [4, 8192, 2], P(None, ('dp', 'expert')), may hold values from 0 to 7, as said below
Outputs:
- router_grad: float32 [4, 8, 4096], P(None, None, 'dp')
- losses: float32 [4, 2], replicated
The draws below stay inside these ranges and needn't reach their ends.
Inputs may be any that keep to these rules, and one draw needn't show every extreme that they name: `expert_ids`: each token names 2 different experts in each layer.
All inputs are finite; a program needn't handle non-finite values.
Results may differ from the reference program's by a relative error of at most 0.0018.
Values sent between devices are 32-bit elements; how exact they have to be, the bound alone decides.
A program may use at most 64 MiB of HBM per device.

```python
import jax
import jax.numpy as jnp
from jax import lax

D = 4096
E = 8
TOP = 2
L = 4
TOKENS = 8192


def draw_hidden_states(key, part):
    first_key = jax.random.fold_in(jax.random.fold_in(key, 11), 0)
    position = jnp.arange(TOKENS, dtype=jnp.float32)
    scale = 0.5 + 1.5 * position / TOKENS
    base = jnp.clip(jax.random.normal(first_key, (L, TOKENS, D), jnp.float32), -4.0, 4.0)
    return (base * scale[None, :, None]).astype(jnp.bfloat16)


def draw_router_weight(key, part):
    first_key, second_key = jax.random.split(jax.random.fold_in(key, 17))
    base = jnp.clip(jax.random.normal(first_key, (L, E, D), jnp.float32), -4.0, 4.0) * D ** (-0.5)
    row_scale = jnp.exp(jax.random.uniform(second_key, (L, E, 1), jnp.float32, -0.69, 0.69))
    return (base * row_scale).astype(jnp.bfloat16)


def draw_expert_ids(key, part):
    keys = jax.random.split(jax.random.fold_in(key, 23), 4)
    favored = jax.random.randint(keys[0], (L, 1), 0, E, jnp.int32)
    position = jnp.arange(TOKENS, dtype=jnp.int32)
    block = position * 16 // TOKENS
    coin = jax.random.randint(keys[1], (L, TOKENS), 0, 16, jnp.int32)
    drawn = jax.random.randint(keys[2], (L, TOKENS), 0, E, jnp.int32)
    first = jnp.where(coin < block[None, :], favored, drawn)
    second = (first + jax.random.randint(keys[3], (L, TOKENS), 1, E, jnp.int32)) % E
    return jnp.stack([first, second], axis=-1).astype(jnp.int32)


def setup_inputs(seed: int = 0) -> dict:
    seeds = jax.random.split(jax.random.key(seed), 4)
    hidden_states = draw_hidden_states(jax.random.fold_in(seeds[3], 71), 0)
    router_weight = draw_router_weight(jax.random.fold_in(seeds[3], 71), 0)
    expert_ids = draw_expert_ids(jax.random.fold_in(seeds[3], 71), 0)
    return {"hidden_states": hidden_states, "router_weight": router_weight, "expert_ids": expert_ids}


balance_coef = 0.02
zloss_coef = 0.001


def layer_terms(states, weight, chosen):
    logits = lax.dot_general(weight, states, (((1,), (1,)), ((), ())), preferred_element_type=jnp.float32)
    expo = jnp.exp(logits)
    total = jnp.sum(expo, axis=0)
    probs = expo / total[None, :]
    lse = jnp.log(total)
    labels = jnp.arange(E, dtype=jnp.int32)[:, None]
    counts = jnp.zeros((E,), jnp.float32)
    for slot in range(TOP):
        counts = counts + jnp.sum((chosen[:, slot][None, :] == labels).astype(jnp.float32), axis=1)
    share = counts / (TOKENS * TOP)
    balance = E * jnp.sum(share * jnp.sum(probs, axis=1) / TOKENS)
    zloss = jnp.sum(lse * lse) / TOKENS
    pull = balance_coef * E * share
    mixed = jnp.sum(probs * pull[:, None], axis=0)
    dlogits = probs * (pull[:, None] - mixed[None, :]) + 2.0 * zloss_coef * lse[None, :] * probs
    dlogits = dlogits.astype(jnp.bfloat16)
    grad = jnp.dot(dlogits, states, preferred_element_type=jnp.float32)
    return grad, jnp.stack([balance, zloss])


def reference(hidden_states, router_weight, expert_ids):
    grads = []
    losses = []
    for layer in range(L):
        grad, pair = layer_terms(hidden_states[layer], router_weight[layer], expert_ids[layer])
        grads.append(grad)
        losses.append(pair)
    return jnp.stack(grads), jnp.stack(losses)
```

```python
import functools

import jax
import jax.numpy as jnp
from jax import lax
from jax.experimental import pallas as pl
from jax.experimental.pallas import tpu as pltpu
from jax.sharding import PartitionSpec as P

balance_coef = 0.02
zloss_coef = 0.001
MESH = pl.DeviceIdType.MESH


def kernel(
    nd, nz, tokens_all,
    x_hbm, w_hbm, ids_hbm, grad_ref, loss_ref,
    x, w, ids, term, recv, zbuf, cnt_d, cnt_z, st_d, st_z,
    x_sem, w_sem, ids_sem, cd_s, cd_r, cz_s, cz_r, sd_s, sd_r, sz_s, sz_r, td_s, td_r, tz_s, tz_r,
):
    layers, rows, _ = x.shape
    experts = w.shape[1]
    picks = ids.shape[1]
    width = term.shape[3]
    me_d = lax.axis_index("dp")
    me_z = lax.axis_index("expert")
    peers_d = [(k, lax.rem(me_d + k, nd)) for k in range(1, nd)]
    peers_z = [(k, lax.rem(me_z + k, nz)) for k in range(1, nz)]

    barrier = pltpu.get_barrier_semaphore()
    for _, peer in peers_z:
        pl.semaphore_signal(barrier, inc=1, device_id={"expert": peer}, device_id_type=MESH)
    for _, peer in peers_d:
        pl.semaphore_signal(barrier, inc=1, device_id={"dp": peer}, device_id_type=MESH)

    ids_copy = pltpu.make_async_copy(ids_hbm, ids, ids_sem)
    ids_copy.start()
    w_copy = pltpu.make_async_copy(w_hbm, w, w_sem)
    w_copy.start()
    pieces = 4 if rows % 64 == 0 else 1
    step = rows // pieces
    for layer in range(layers):
        for piece in range(pieces):
            part = pl.ds(piece * step, step)
            pltpu.make_async_copy(x_hbm.at[layer, part], x.at[layer, part], x_sem.at[layer]).start()

    def exchange(axis, peers, buf, me, send_sem, recv_sem):
        copies = []
        for k, peer in peers:
            copy = pltpu.make_async_remote_copy(
                src_ref=buf.at[me],
                dst_ref=buf.at[me],
                send_sem=send_sem.at[k - 1],
                recv_sem=recv_sem,
                device_id={axis: peer},
                device_id_type=MESH,
            )
            copy.start()
            copies.append(copy)
        return copies

    def arrived(buf, count, sem):
        part = buf.at[pl.ds(0, count)]
        pltpu.make_async_copy(part, part, sem).wait()

    def total_of(buf, count):
        out = buf[0]
        for i in range(1, count):
            out = out + buf[i]
        return out

    labels = lax.broadcasted_iota(jnp.int32, (experts, rows), 0)
    lane = lax.broadcasted_iota(jnp.int32, cnt_d.shape[1:], 1)
    ids_copy.wait()
    counts = jnp.zeros(cnt_d.shape[1:], jnp.float32)
    for layer in range(layers):
        hits = jnp.zeros((experts, rows), jnp.float32)
        for slot in range(picks):
            chosen = ids[layer, pl.ds(slot, 1), :]
            hits = hits + (jnp.broadcast_to(chosen, labels.shape) == labels).astype(jnp.float32)
        counts = jnp.where(lane == layer, jnp.sum(hits, axis=1, keepdims=True), counts)
    cnt_d[me_d] = counts

    probs, lses = [], []

    def forward(layer):
        pltpu.make_async_copy(x_hbm.at[layer], x.at[layer], x_sem.at[layer]).wait()
        logits = lax.dot_general(
            w[layer], x[layer], (((1,), (1,)), ((), ())), preferred_element_type=jnp.float32
        )
        expo = jnp.exp(logits)
        total = jnp.sum(expo, axis=0, keepdims=True)
        probs.append(expo / total)
        lses.append(jnp.log(total))

    w_copy.wait()
    pending = []
    wait_at = max(layers - 2, 0)
    for layer in range(layers):
        forward(layer)
        if layer == 0:
            pl.semaphore_wait(barrier, nd + nz - 2)
            pending += exchange("dp", peers_d, cnt_d, me_d, cd_s, cd_r)
        if layer == wait_at:
            arrived(cnt_d, nd - 1, cd_r)
            cnt_z[me_z] = total_of(cnt_d, nd)
            pending += exchange("expert", peers_z, cnt_z, me_z, cz_s, cz_r)
    arrived(cnt_z, nz - 1, cz_r)
    share = total_of(cnt_z, nz) / (tokens_all * picks)

    def combine(layer):
        arrived(recv.at[layer], nd - 1, td_r.at[layer])
        out = term[layer, me_d]
        for k in range(nd - 1):
            out = out + recv[layer, k]
        zbuf[layer, me_z] = out
        return exchange("expert", peers_z, zbuf.at[layer], me_z, tz_s.at[layer], tz_r.at[layer])

    row = lax.broadcasted_iota(jnp.int32, cnt_d.shape[1:], 0)
    stats = jnp.zeros(cnt_d.shape[1:], jnp.float32)
    for layer in range(layers):
        share_l = share[:, layer:layer + 1]
        pull = balance_coef * experts * share_l
        mixed = jnp.sum(probs[layer] * pull, axis=0, keepdims=True)
        dlogits = probs[layer] * (pull - mixed) + 2.0 * zloss_coef * lses[layer] * probs[layer]
        dlogits = dlogits.astype(jnp.bfloat16)
        for d in range(nd):
            term[layer, d] = jnp.dot(
                dlogits, x[layer, :, d * width:(d + 1) * width], preferred_element_type=jnp.float32
            )
        for k, peer in peers_d:
            copy = pltpu.make_async_remote_copy(
                src_ref=term.at[layer, peer],
                dst_ref=recv.at[layer, k - 1],
                send_sem=td_s.at[layer, k - 1],
                recv_sem=td_r.at[layer],
                device_id={"dp": peer},
                device_id_type=MESH,
            )
            copy.start()
            pending.append(copy)
        prob_sum = jnp.sum(probs[layer], axis=1, keepdims=True)
        balance = experts * jnp.sum(share_l * prob_sum / tokens_all, axis=0, keepdims=True)
        zloss = jnp.sum(lses[layer] * lses[layer], axis=1, keepdims=True) / tokens_all
        stats = jnp.where((row == layer) & (lane == 0), balance, stats)
        stats = jnp.where((row == layer) & (lane == 1), zloss, stats)
        if layer >= 2:
            pending += combine(layer - 2)
    st_d[me_d] = stats
    pending += exchange("dp", peers_d, st_d, me_d, sd_s, sd_r)
    for layer in range(max(layers - 2, 0), layers):
        pending += combine(layer)
    arrived(st_d, nd - 1, sd_r)
    st_z[me_z] = total_of(st_d, nd)
    pending += exchange("expert", peers_z, st_z, me_z, sz_s, sz_r)
    for layer in range(layers):
        arrived(zbuf.at[layer], nz - 1, tz_r.at[layer])
        grad_ref[layer] = total_of(zbuf.at[layer], nz)
    arrived(st_z, nz - 1, sz_r)
    loss_ref[...] = total_of(st_z, nz)
    for copy in pending:
        copy.wait_send()


def on_device(nd, nz, hidden_states, router_weight, expert_ids):
    layers, rows, depth = hidden_states.shape
    experts = router_weight.shape[1]
    picks = expert_ids.shape[2]
    width = depth // nd
    tokens_all = rows * nd * nz
    tile = (max(8, experts, layers), 128)
    dma = pltpu.SemaphoreType.DMA
    anywhere = pl.BlockSpec(memory_space=pl.ANY)
    inside = pl.BlockSpec(memory_space=pltpu.VMEM)
    grad, loss = pl.pallas_call(
        functools.partial(kernel, nd, nz, tokens_all),
        out_shape=(
            jax.ShapeDtypeStruct((layers, experts, width), jnp.float32),
            jax.ShapeDtypeStruct(tile, jnp.float32),
        ),
        in_specs=[anywhere] * 3,
        out_specs=(inside, inside),
        scratch_shapes=[
            pltpu.VMEM(hidden_states.shape, jnp.bfloat16),
            pltpu.VMEM(router_weight.shape, jnp.bfloat16),
            pltpu.VMEM((layers, picks, rows), jnp.int32),
            pltpu.VMEM((layers, nd, experts, width), jnp.float32),
            pltpu.VMEM((layers, nd - 1, experts, width), jnp.float32),
            pltpu.VMEM((layers, nz, experts, width), jnp.float32),
            pltpu.VMEM((nd,) + tile, jnp.float32),
            pltpu.VMEM((nz,) + tile, jnp.float32),
            pltpu.VMEM((nd,) + tile, jnp.float32),
            pltpu.VMEM((nz,) + tile, jnp.float32),
            dma((layers,)), dma, dma,
            dma((nd - 1,)), dma, dma((nz - 1,)), dma,
            dma((nd - 1,)), dma, dma((nz - 1,)), dma,
            dma((layers, nd - 1)), dma((layers,)), dma((layers, nz - 1)), dma((layers,)),
        ],
        compiler_params=pltpu.CompilerParams(collective_id=0, has_side_effects=True),
    )(hidden_states, router_weight, jnp.transpose(expert_ids, (0, 2, 1)))
    return grad, loss[:layers, :2]


def solution(mesh):
    in_specs = (P(None, ("dp", "expert"), None), P(), P(None, ("dp", "expert"), None))
    out_specs = (P(None, None, "dp"), P())
    return jax.shard_map(
        functools.partial(on_device, mesh.shape["dp"], mesh.shape["expert"]),
        mesh=mesh, in_specs=in_specs, out_specs=out_specs, check_vma=False,
    )
```

```python
import functools

import jax
import jax.numpy as jnp
from jax import lax
from jax.experimental import pallas as pl
from jax.experimental.pallas import tpu as pltpu
from jax.sharding import PartitionSpec as P

balance_coef = 0.02
zloss_coef = 0.001
MESH = pl.DeviceIdType.MESH


def kernel(
    nd, nz, tokens_all,
    x_hbm, w_hbm, ids_hbm, grad_ref, loss_ref,
    x, w, ids, term, half, part_sum, recv, zbuf, cnt_d, cnt_z, st_d, st_z,
    x_sem, w_sem, ids_sem, cd_s, cd_r, cz_s, cz_r, sd_s, sd_r, sz_s, sz_r,
    tp_s, tp_r, td_s, td_r, tz_s, tz_r,
):
    layers, rows, _ = x.shape
    experts = w.shape[1]
    picks = ids.shape[1]
    width = term.shape[4]
    chips = nd // 2
    me_d = lax.axis_index("dp")
    me_z = lax.axis_index("expert")
    peers_d = [(k, lax.rem(me_d + k, nd)) for k in range(1, nd)]
    core, chip = lax.rem(me_d, 2), me_d // 2
    partner = me_d + 1 - 2 * core
    peers_c = [(k, lax.rem(chip + k, chips)) for k in range(1, chips)]
    peers_z = [(k, lax.rem(me_z + k, nz)) for k in range(1, nz)]

    barrier = pltpu.get_barrier_semaphore()
    for _, peer in peers_z:
        pl.semaphore_signal(barrier, inc=1, device_id={"expert": peer}, device_id_type=MESH)
    for _, peer in peers_d:
        pl.semaphore_signal(barrier, inc=1, device_id={"dp": peer}, device_id_type=MESH)

    ids_copy = pltpu.make_async_copy(ids_hbm, ids, ids_sem)
    ids_copy.start()
    w_copy = pltpu.make_async_copy(w_hbm, w, w_sem)
    w_copy.start()
    pieces = 4 if rows % 64 == 0 else 1
    step = rows // pieces
    for layer in range(layers):
        for piece in range(pieces):
            part = pl.ds(piece * step, step)
            pltpu.make_async_copy(x_hbm.at[layer, part], x.at[layer, part], x_sem.at[layer]).start()

    def exchange(axis, peers, buf, me, send_sem, recv_sem):
        copies = []
        for k, peer in peers:
            copy = pltpu.make_async_remote_copy(
                src_ref=buf.at[me],
                dst_ref=buf.at[me],
                send_sem=send_sem.at[k - 1],
                recv_sem=recv_sem,
                device_id={axis: peer},
                device_id_type=MESH,
            )
            copy.start()
            copies.append(copy)
        return copies

    def arrived(buf, count, sem):
        part = buf.at[pl.ds(0, count)]
        pltpu.make_async_copy(part, part, sem).wait()

    def total_of(buf, count):
        out = buf[0]
        for i in range(1, count):
            out = out + buf[i]
        return out

    labels = lax.broadcasted_iota(jnp.int32, (experts, rows), 0)
    lane = lax.broadcasted_iota(jnp.int32, cnt_d.shape[1:], 1)
    ids_copy.wait()
    counts = jnp.zeros(cnt_d.shape[1:], jnp.float32)
    for layer in range(layers):
        hits = jnp.zeros((experts, rows), jnp.float32)
        for slot in range(picks):
            chosen = ids[layer, pl.ds(slot, 1), :]
            hits = hits + (jnp.broadcast_to(chosen, labels.shape) == labels).astype(jnp.float32)
        counts = jnp.where(lane == layer, jnp.sum(hits, axis=1, keepdims=True), counts)
    cnt_d[me_d] = counts

    probs, lses = [], []

    def forward(layer):
        pltpu.make_async_copy(x_hbm.at[layer], x.at[layer], x_sem.at[layer]).wait()
        logits = lax.dot_general(
            w[layer], x[layer], (((1,), (1,)), ((), ())), preferred_element_type=jnp.float32
        )
        expo = jnp.exp(logits)
        total = jnp.sum(expo, axis=0, keepdims=True)
        probs.append(expo / total)
        lses.append(jnp.log(total))

    pl.semaphore_wait(barrier, nd + nz - 2)
    pending = exchange("dp", peers_d, cnt_d, me_d, cd_s, cd_r)
    w_copy.wait()
    wait_at = min(1, layers - 1)
    for layer in range(layers):
        forward(layer)
        if layer == wait_at:
            arrived(cnt_d, nd - 1, cd_r)
            cnt_z[me_z] = total_of(cnt_d, nd)
            pending += exchange("expert", peers_z, cnt_z, me_z, cz_s, cz_r)
    arrived(cnt_z, nz - 1, cz_r)
    share = total_of(cnt_z, nz) / (tokens_all * picks)

    def half_term(layer, dlogits, parity):
        for c in range(chips):
            at = (2 * c + parity) * width
            at = pl.multiple_of(at, 128)
            term[layer, parity, c] = jnp.dot(
                dlogits, x[layer, :, pl.ds(at, width)], preferred_element_type=jnp.float32
            )

    to_partner = []
    for layer in range(layers):
        pull = balance_coef * experts * share[:, layer:layer + 1]
        mixed = jnp.sum(probs[layer] * pull, axis=0, keepdims=True)
        dlogits = probs[layer] * (pull - mixed) + 2.0 * zloss_coef * lses[layer] * probs[layer]
        dlogits = dlogits.astype(jnp.bfloat16)
        half_term(layer, dlogits, 1 - core)
        copy = pltpu.make_async_remote_copy(
            src_ref=term.at[layer, 1 - core],
            dst_ref=half.at[layer],
            send_sem=tp_s.at[layer],
            recv_sem=tp_r.at[layer],
            device_id={"dp": partner},
            device_id_type=MESH,
        )
        copy.start()
        to_partner.append(copy)
        half_term(layer, dlogits, core)

    for layer in range(layers):
        to_partner[layer].wait_recv()
        for c in range(chips):
            part_sum[layer, c] = term[layer, core, c] + half[layer, c]
        for k, peer in peers_c:
            copy = pltpu.make_async_remote_copy(
                src_ref=part_sum.at[layer, peer],
                dst_ref=recv.at[layer, k - 1],
                send_sem=td_s.at[layer, k - 1],
                recv_sem=td_r.at[layer],
                device_id={"dp": 2 * peer + core},
                device_id_type=MESH,
            )
            copy.start()
            pending.append(copy)
    pending += to_partner

    row = lax.broadcasted_iota(jnp.int32, cnt_d.shape[1:], 0)
    stats = jnp.zeros(cnt_d.shape[1:], jnp.float32)
    for layer in range(layers):
        share_l = share[:, layer:layer + 1]
        prob_sum = jnp.sum(probs[layer], axis=1, keepdims=True)
        balance = experts * jnp.sum(share_l * prob_sum / tokens_all, axis=0, keepdims=True)
        zloss = jnp.sum(lses[layer] * lses[layer], axis=1, keepdims=True) / tokens_all
        stats = jnp.where((row == 0) & (lane == layer), balance, stats)
        stats = jnp.where((row == 1) & (lane == layer), zloss, stats)
    st_d[me_d] = stats
    pending += exchange("dp", peers_d, st_d, me_d, sd_s, sd_r)
    for layer in range(layers):
        if layer == layers - 1:
            arrived(st_d, nd - 1, sd_r)
            st_z[me_z] = total_of(st_d, nd)
            pending += exchange("expert", peers_z, st_z, me_z, sz_s, sz_r)
        arrived(recv.at[layer], chips - 1, td_r.at[layer])
        out = part_sum[layer, chip]
        for k in range(chips - 1):
            out = out + recv[layer, k]
        zbuf[layer, me_z] = out
        pending += exchange(
            "expert", peers_z, zbuf.at[layer], me_z, tz_s.at[layer], tz_r.at[layer]
        )
    for layer in range(layers):
        arrived(zbuf.at[layer], nz - 1, tz_r.at[layer])
        grad_ref[layer] = total_of(zbuf.at[layer], nz)
    arrived(st_z, nz - 1, sz_r)
    loss_ref[...] = total_of(st_z, nz)[:2, :layers]
    for copy in pending:
        copy.wait_send()


def on_device(nd, nz, hidden_states, router_weight, expert_ids):
    layers, rows, depth = hidden_states.shape
    experts = router_weight.shape[1]
    picks = expert_ids.shape[2]
    width = depth // nd
    chips = nd // 2
    tokens_all = rows * nd * nz
    tile = (max(8, experts), 128)
    dma = pltpu.SemaphoreType.DMA
    anywhere = pl.BlockSpec(memory_space=pl.ANY)
    inside = pl.BlockSpec(memory_space=pltpu.VMEM)
    grad, loss = pl.pallas_call(
        functools.partial(kernel, nd, nz, tokens_all),
        out_shape=(
            pltpu.VMEM((layers, experts, width), jnp.float32),
            pltpu.VMEM((2, layers), jnp.float32),
        ),
        in_specs=[anywhere] * 3,
        out_specs=(inside, inside),
        scratch_shapes=[
            pltpu.VMEM(hidden_states.shape, jnp.bfloat16),
            pltpu.VMEM(router_weight.shape, jnp.bfloat16),
            pltpu.VMEM((layers, picks, rows), jnp.int32),
            pltpu.VMEM((layers, 2, chips, experts, width), jnp.float32),
            pltpu.VMEM((layers, chips, experts, width), jnp.float32),
            pltpu.VMEM((layers, chips, experts, width), jnp.float32),
            pltpu.VMEM((layers, chips - 1, experts, width), jnp.float32),
            pltpu.VMEM((layers, nz, experts, width), jnp.float32),
            pltpu.VMEM((nd,) + tile, jnp.float32),
            pltpu.VMEM((nz,) + tile, jnp.float32),
            pltpu.VMEM((nd,) + tile, jnp.float32),
            pltpu.VMEM((nz,) + tile, jnp.float32),
            dma((layers,)), dma, dma,
            dma((nd - 1,)), dma, dma((nz - 1,)), dma,
            dma((nd - 1,)), dma, dma((nz - 1,)), dma,
            dma((layers,)), dma((layers,)),
            dma((layers, chips - 1)), dma((layers,)), dma((layers, nz - 1)), dma((layers,)),
        ],
        compiler_params=pltpu.CompilerParams(collective_id=0, has_side_effects=True),
    )(hidden_states, router_weight, jnp.transpose(expert_ids, (0, 2, 1)))
    return grad, jnp.transpose(loss)


def solution(mesh):
    in_specs = (P(None, ("dp", "expert"), None), P(), P(None, ("dp", "expert"), None))
    out_specs = (P(None, None, "dp"), P())
    return jax.shard_map(
        functools.partial(on_device, mesh.shape["dp"], mesh.shape["expert"]),
        mesh=mesh, in_specs=in_specs, out_specs=out_specs, check_vma=False,
    )
```

```python
import functools

import jax
import jax.numpy as jnp
from jax import lax
from jax.experimental import pallas as pl
from jax.experimental.pallas import tpu as pltpu
from jax.sharding import PartitionSpec as P

balance_coef = 0.02
zloss_coef = 0.001
MESH = pl.DeviceIdType.MESH


def kernel(
    nd, nz, tokens_all,
    x_hbm, w_hbm, ids_hbm, grad_ref, loss_ref,
    x, w, ids, term, half, part_sum, recv, zbuf, cnt_d, cnt_z, st_d, st_z,
    x_sem, w_sem, ids_sem, cd_s, cd_r, cz_s, cz_r, sd_s, sd_r, sz_s, sz_r,
    tp_s, tp_r, td_s, td_r, tz_s, tz_r,
):
    layers, rows, _ = x.shape
    experts = w.shape[1]
    picks = ids.shape[1]
    width = term.shape[4]
    chips = nd // 2
    me_d = lax.axis_index("dp")
    me_z = lax.axis_index("expert")
    peers_d = [(k, lax.rem(me_d + k, nd)) for k in range(1, nd)]
    core, chip = lax.rem(me_d, 2), me_d // 2
    partner = me_d + 1 - 2 * core
    peers_c = [(k, lax.rem(chip + k, chips)) for k in range(1, chips)]
    peers_z = [(k, lax.rem(me_z + k, nz)) for k in range(1, nz)]

    barrier = pltpu.get_barrier_semaphore()
    for _, peer in peers_z:
        pl.semaphore_signal(barrier, inc=1, device_id={"expert": peer}, device_id_type=MESH)
    for _, peer in peers_d:
        pl.semaphore_signal(barrier, inc=1, device_id={"dp": peer}, device_id_type=MESH)

    ids_copy = pltpu.make_async_copy(ids_hbm, ids, ids_sem)
    ids_copy.start()
    w_copy = pltpu.make_async_copy(w_hbm, w, w_sem)
    w_copy.start()
    pieces = 4 if rows % 64 == 0 else 1
    step = rows // pieces
    for layer in range(layers):
        for piece in range(pieces):
            part = pl.ds(piece * step, step)
            pltpu.make_async_copy(x_hbm.at[layer, part], x.at[layer, part], x_sem.at[layer]).start()

    def exchange(axis, peers, buf, me, send_sem, recv_sem):
        copies = []
        for k, peer in peers:
            copy = pltpu.make_async_remote_copy(
                src_ref=buf.at[me],
                dst_ref=buf.at[me],
                send_sem=send_sem.at[k - 1],
                recv_sem=recv_sem,
                device_id={axis: peer},
                device_id_type=MESH,
            )
            copy.start()
            copies.append(copy)
        return copies

    def arrived(buf, count, sem):
        part = buf.at[pl.ds(0, count)]
        pltpu.make_async_copy(part, part, sem).wait()

    def total_of(buf, count):
        out = buf[0]
        for i in range(1, count):
            out = out + buf[i]
        return out

    labels = lax.broadcasted_iota(jnp.int32, (experts, rows), 0)
    lanes = cnt_d.shape[2]
    lane = lax.broadcasted_iota(jnp.int32, (experts, lanes), 1)
    row = lax.broadcasted_iota(jnp.int32, (experts, lanes), 0)
    ids_copy.wait()
    counts = jnp.zeros((experts, lanes), jnp.float32)
    for layer in range(layers):
        hits = jnp.zeros((experts, rows), jnp.float32)
        for slot in range(picks):
            chosen = ids[layer, pl.ds(slot, 1), :]
            hits = hits + (jnp.broadcast_to(chosen, labels.shape) == labels).astype(jnp.float32)
        counts = jnp.where(lane == layer * experts + row, jnp.sum(hits, axis=1, keepdims=True), counts)
    cnt_d[me_d] = jnp.sum(counts, axis=0, keepdims=True)

    probs, lses = [], []

    def forward(layer):
        pltpu.make_async_copy(x_hbm.at[layer], x.at[layer], x_sem.at[layer]).wait()
        logits = lax.dot_general(
            w[layer], x[layer], (((1,), (1,)), ((), ())), preferred_element_type=jnp.float32
        )
        expo = jnp.exp(logits)
        total = jnp.sum(expo, axis=0, keepdims=True)
        probs.append(expo / total)
        lses.append(jnp.log(total))

    pl.semaphore_wait(barrier, nd + nz - 2)
    pending = exchange("dp", peers_d, cnt_d, me_d, cd_s, cd_r)
    w_copy.wait()
    wait_at = min(1, layers - 1)
    for layer in range(layers):
        forward(layer)
        if layer == wait_at:
            arrived(cnt_d, nd - 1, cd_r)
            cnt_z[me_z] = total_of(cnt_d, nd)
            pending += exchange("expert", peers_z, cnt_z, me_z, cz_s, cz_r)
    arrived(cnt_z, nz - 1, cz_r)
    share_row = total_of(cnt_z, nz) / (tokens_all * picks)
    shares = [
        jnp.sum(jnp.where(lane == layer * experts + row, share_row, 0.0), axis=1, keepdims=True)
        for layer in range(layers)
    ]

    def half_term(layer, dlogits, parity):
        for c in range(chips):
            at = (2 * c + parity) * width
            at = pl.multiple_of(at, 128)
            term[layer, parity, c] = jnp.dot(
                dlogits, x[layer, :, pl.ds(at, width)], preferred_element_type=jnp.float32
            )

    to_partner = []
    for layer in range(layers):
        pull = balance_coef * experts * shares[layer]
        mixed = jnp.sum(probs[layer] * pull, axis=0, keepdims=True)
        dlogits = probs[layer] * (pull - mixed) + 2.0 * zloss_coef * lses[layer] * probs[layer]
        dlogits = dlogits.astype(jnp.bfloat16)
        half_term(layer, dlogits, 1 - core)
        copy = pltpu.make_async_remote_copy(
            src_ref=term.at[layer, 1 - core],
            dst_ref=half.at[layer],
            send_sem=tp_s.at[layer],
            recv_sem=tp_r.at[layer],
            device_id={"dp": partner},
            device_id_type=MESH,
        )
        copy.start()
        to_partner.append(copy)
        half_term(layer, dlogits, core)

    for layer in range(layers):
        to_partner[layer].wait_recv()
        for c in range(chips):
            part_sum[layer, c] = term[layer, core, c] + half[layer, c]
        for k, peer in peers_c:
            copy = pltpu.make_async_remote_copy(
                src_ref=part_sum.at[layer, peer],
                dst_ref=recv.at[layer, k - 1],
                send_sem=td_s.at[layer, k - 1],
                recv_sem=td_r.at[layer],
                device_id={"dp": 2 * peer + core},
                device_id_type=MESH,
            )
            copy.start()
            pending.append(copy)
    pending += to_partner

    line = lax.broadcasted_iota(jnp.int32, (1, lanes), 1)
    stats = jnp.zeros((1, lanes), jnp.float32)
    for layer in range(layers):
        prob_sum = jnp.sum(probs[layer], axis=1, keepdims=True)
        balance = experts * jnp.sum(shares[layer] * prob_sum / tokens_all, axis=0, keepdims=True)
        zloss = jnp.sum(lses[layer] * lses[layer], axis=1, keepdims=True) / tokens_all
        stats = jnp.where(line == layer, balance, stats)
        stats = jnp.where(line == layers + layer, zloss, stats)
    st_d[me_d] = stats
    pending += exchange("dp", peers_d, st_d, me_d, sd_s, sd_r)
    for layer in range(layers):
        if layer == layers - 1:
            arrived(st_d, nd - 1, sd_r)
            st_z[me_z] = total_of(st_d, nd)
            pending += exchange("expert", peers_z, st_z, me_z, sz_s, sz_r)
        arrived(recv.at[layer], chips - 1, td_r.at[layer])
        out = part_sum[layer, chip]
        for k in range(chips - 1):
            out = out + recv[layer, k]
        zbuf[layer, me_z] = out
        pending += exchange(
            "expert", peers_z, zbuf.at[layer], me_z, tz_s.at[layer], tz_r.at[layer]
        )
    for layer in range(layers):
        arrived(zbuf.at[layer], nz - 1, tz_r.at[layer])
        grad_ref[layer] = total_of(zbuf.at[layer], nz)
    arrived(st_z, nz - 1, sz_r)
    losses = total_of(st_z, nz)
    loss_ref[0:1] = losses[:, :layers]
    loss_ref[1:2] = losses[:, layers:2 * layers]
    for copy in pending:
        copy.wait_send()


def on_device(nd, nz, hidden_states, router_weight, expert_ids):
    layers, rows, depth = hidden_states.shape
    experts = router_weight.shape[1]
    picks = expert_ids.shape[2]
    width = depth // nd
    chips = nd // 2
    tokens_all = rows * nd * nz
    tile = (1, pl.cdiv(layers * experts, 128) * 128)
    dma = pltpu.SemaphoreType.DMA
    anywhere = pl.BlockSpec(memory_space=pl.ANY)
    inside = pl.BlockSpec(memory_space=pltpu.VMEM)
    grad, loss = pl.pallas_call(
        functools.partial(kernel, nd, nz, tokens_all),
        out_shape=(
            pltpu.VMEM((layers, experts, width), jnp.float32),
            pltpu.VMEM((2, layers), jnp.float32),
        ),
        in_specs=[anywhere] * 3,
        out_specs=(inside, inside),
        scratch_shapes=[
            pltpu.VMEM(hidden_states.shape, jnp.bfloat16),
            pltpu.VMEM(router_weight.shape, jnp.bfloat16),
            pltpu.VMEM((layers, picks, rows), jnp.int32),
            pltpu.VMEM((layers, 2, chips, experts, width), jnp.float32),
            pltpu.VMEM((layers, chips, experts, width), jnp.float32),
            pltpu.VMEM((layers, chips, experts, width), jnp.float32),
            pltpu.VMEM((layers, chips - 1, experts, width), jnp.float32),
            pltpu.VMEM((layers, nz, experts, width), jnp.float32),
            pltpu.VMEM((nd,) + tile, jnp.float32),
            pltpu.VMEM((nz,) + tile, jnp.float32),
            pltpu.VMEM((nd,) + tile, jnp.float32),
            pltpu.VMEM((nz,) + tile, jnp.float32),
            dma((layers,)), dma, dma,
            dma((nd - 1,)), dma, dma((nz - 1,)), dma,
            dma((nd - 1,)), dma, dma((nz - 1,)), dma,
            dma((layers,)), dma((layers,)),
            dma((layers, chips - 1)), dma((layers,)), dma((layers, nz - 1)), dma((layers,)),
        ],
        compiler_params=pltpu.CompilerParams(collective_id=0, has_side_effects=True),
    )(hidden_states, router_weight, jnp.transpose(expert_ids, (0, 2, 1)))
    return grad, jnp.transpose(loss)


def solution(mesh):
    in_specs = (P(None, ("dp", "expert"), None), P(), P(None, ("dp", "expert"), None))
    out_specs = (P(None, None, "dp"), P())
    return jax.shard_map(
        functools.partial(on_device, mesh.shape["dp"], mesh.shape["expert"]),
        mesh=mesh, in_specs=in_specs, out_specs=out_specs, check_vma=False,
    )
```
